32 devices in a mesh: groups: 2 (over y), rows: 16 (over z, x, core).
Axes of the slice: x: 2, y: 2, z: 4, core: 2. Of those that a mesh axis runs over, the one named last changes fastest.
Arguments:
- pair_repr: bfloat16 [256, 128, 128], P('groups', 'rows'), parts along dimension 0, may hold values from -6 to 6
- single_repr: bfloat16 [256, 384], P(('groups', 'rows')), parts along dimension 0, may hold values from -6 to 6
- residue_index: int32 [256], P('groups'), parts along dimension 0, may hold values from 0 to 47
- chain_index: int32 [256], P('groups'), parts along dimension 0, may hold values from 0 to 3
- complex_index: int32 [256], P('groups'), parts along dimension 0, may hold values from 0 to 7, never falling along the last dimension, each value on 1 to 96 neighbouring positions
- pad_mask: int32 [256], P('groups'), parts along dimension 0, may hold values 0 or 1
- w_query: bfloat16 [384, 384], replicated, may hold values from -3 to 3
- w_key: bfloat16 [384, 384], replicated, may hold values from -3.1 to 3.1
- w_value: bfloat16 [384, 384], replicated, may hold values from -0.3125 to 0.3125
- w_gate: bfloat16 [384, 384], replicated, may hold values from -0.3125 to 0.3125
- w_out: bfloat16 [384, 384], replicated, may hold values from -2.5 to 2.5
- w_bias: bfloat16 [128, 16], replicated, may hold values from -0.5 to 0.5
- rel_table: bfloat16 [66, 128], replicated, may hold values from -6 to 6
- w_mix_a: bfloat16 [384, 128], replicated, may hold values from -0.3125 to 0.3125
- w_mix_b: bfloat16 [384, 128], replicated, may hold values from -0.3125 to 0.3125
- w_hidden_a: bfloat16 [128, 512], replicated, may hold values from -0.5 to 0.5
- w_hidden_b: bfloat16 [128, 512], replicated, may hold values from -0.5 to 0.5
- w_hidden_out: bfloat16 [512, 128], replicated, may hold values from -0.25 to 0.25
- w_pae: bfloat16 [128, 64], replicated, may hold values from -30 to 30
- pae_bias: float32 [64], replicated, may hold values from -4 to 4
Outputs:
- refined: bfloat16 [256, 384], P(('groups', 'rows')), parts along dimension 0
- errors: float32 [256, 128], P(('groups', 'rows')), parts along dimension 0
The draws below stay inside these ranges and needn't reach their ends.
There are 2 independent parts, one for each index of `groups`. The reference program is written for one: setup_inputs(seed, part) draws one part's arguments, and reference() takes and returns one part's arrays. A program takes and returns all parts, laid end to end along the dimension named above; an argument that names none is the same for every part. Nothing has to cross between parts.
Inputs may be any that keep to these rules, and one draw needn't show every extreme that they name: `complex_index`: never falls along the tokens; each complex holds 1 to 96 consecutive tokens.
All inputs are finite; a program needn't handle non-finite values.
Results may differ from the reference program's by a relative error of at most 0.023.
Values may be sent and summed in bfloat16 or wider, within the bound.
A program may use at most 128 MiB of HBM per device.

```python
import math
import jax
import jax.numpy as jnp
import numpy as np
from jax import lax

C = 128
S = 384
HEADS = 16
BINS = 64
FFN = 512
TOK_DEV = 8
N = 128
REL_BINS = 66


def query_key_pair(key):
    base = jax.random.normal(jax.random.fold_in(key, 101), (S, S), jnp.float32)
    other = jax.random.normal(jax.random.fold_in(key, 202), (S, S), jnp.float32)
    return (jnp.clip(base, -6.0, 6.0) * (2.0 * S ** (-0.5)), jnp.clip(other, -6.0, 6.0) * (2.0 * S ** (-0.5)))


def draw_w_query(key, part):
    return query_key_pair(key)[0].astype(jnp.bfloat16)


def draw_w_key(key, part):
    return query_key_pair(key)[1].astype(jnp.bfloat16)


def draw_w_pae(key, part):
    base = jax.random.normal(jax.random.fold_in(key, 404), (C, BINS), jnp.float32)
    return (jnp.clip(base, -6.0, 6.0) * C ** (-0.5)).astype(jnp.bfloat16)


def plant(array, own_key, least, largest):
    longest = array.shape.index(max(array.shape))
    spots = []
    for shift in (0, 1):
        where = [jax.random.randint(jax.random.fold_in(own_key, axis), (), 0, length) for axis, length in enumerate(array.shape)]
        where[longest] = (where[longest] + shift) % array.shape[longest]
        spots.append(tuple(where))
    return array.at[spots[0]].set(least).at[spots[1]].set(largest)


def shard_levels(own_key, dims, pieces, low, high):
    level = 1.0
    for position, parts in pieces:
        draws = jax.random.uniform(jax.random.fold_in(jax.random.fold_in(own_key, 6), position), (parts,), jnp.float32, low / len(pieces), high / len(pieces))
        level = level * jnp.repeat(jnp.exp(draws), dims[position] // parts).reshape((-1,) + (1,) * (len(dims) - 1 - position))
    return level


def split_up(count, total, most, slope):
    loads = [(1 << 20) // math.isqrt(standing ** slope) + 1 for standing in range(2, count + 1)]
    surplus, counts = total - most - (count - 1), [1] * (count - 1)
    while surplus > 0:
        candidates = [i for i in range(count - 1) if counts[i] < most]
        mass, remaining = sum([loads[i] for i in candidates]), surplus
        for i in candidates:
            addition = min(most - counts[i], max(1, remaining * loads[i] // mass), surplus)
            counts[i] = counts[i] + addition
            surplus = surplus - addition
    return np.array([most] + counts)


def ragged_sizes(own_key, amount, total, most, lean):
    if amount == 2:
        one = jax.random.randint(own_key, (), max(1, total - most), min(most, total - 1) + 1)
        return jnp.stack([one, total - one])
    sizes = jnp.asarray(split_up(amount, total, most, lean), jnp.int32)
    twos = (amount - 1) // 2
    giver, receiver = sizes[1:1 + 2 * twos:2], sizes[2:2 + 2 * twos:2]
    margin = jnp.minimum(giver - 1, most - receiver)
    moved = jax.random.randint(jax.random.fold_in(own_key, 1), (twos,), 0, 1 << 20) % (margin + 1)
    sizes = sizes.at[1:1 + 2 * twos:2].set(giver - moved).at[2:2 + 2 * twos:2].set(receiver + moved)
    return sizes[jax.random.permutation(jax.random.fold_in(own_key, 2), amount)]


def gaussian(stream_key, shape, scale, most, shards=(), kind=jnp.bfloat16):
    gain = shard_levels(stream_key, shape, shards, -0.22, 0.18) if shards else 1.0
    array = jax.random.normal(stream_key, shape, jnp.float32) * scale * gain
    return jnp.minimum(jnp.maximum(array, -most), most).astype(kind)


def setup_inputs(seed: int = 0, part: int = 0) -> dict:
    streams_of = jax.random.split(jax.random.key(seed), 21)
    part_splits = jax.random.split(jax.random.fold_in(streams_of[20], part), 21)
    pair_repr = gaussian(part_splits[0], (N, N, C), 1.0, 6.0, ((1, 16),))
    single_repr = gaussian(part_splits[1], (N, S), 1.0, 6.0, ((0, 16),))
    residue_index = plant(jax.random.randint(part_splits[2], (N,), 0, 48), jax.random.fold_in(part_splits[2], 1), 0, 47).astype(jnp.int32)
    chain_index = plant(jax.random.randint(part_splits[3], (N,), 0, 4), jax.random.fold_in(part_splits[3], 1), 0, 3).astype(jnp.int32)
    complex_index = jnp.searchsorted(jnp.cumsum(ragged_sizes(part_splits[4], 8, N, 3 * N // 4, 1)), jnp.arange(N), side="right").astype(jnp.int32)
    pad_mask = plant((jax.random.randint(part_splits[5], (N,), 0, 8) < 7).astype(jnp.int32), jax.random.fold_in(part_splits[5], 1), 0, 1)
    w_query = draw_w_query(jax.random.fold_in(streams_of[20], 71), part)
    w_key = draw_w_key(jax.random.fold_in(streams_of[20], 71), part)
    w_value = gaussian(streams_of[8], (S, S), S ** -0.5, 0.3125)
    w_gate = gaussian(streams_of[9], (S, S), S ** -0.5, 0.3125)
    w_out = gaussian(streams_of[10], (S, S), (max(S // 64, 1)) ** -0.5, 2.5)
    w_bias = gaussian(streams_of[11], (C, HEADS), C ** -0.5, 0.5)
    rel_table = gaussian(streams_of[12], (REL_BINS, C), 1.0, 6.0)
    w_mix_a = gaussian(streams_of[13], (S, C), S ** -0.5, 0.3125)
    w_mix_b = gaussian(streams_of[14], (S, C), S ** -0.5, 0.3125)
    w_hidden_a = gaussian(streams_of[15], (C, FFN), C ** -0.5, 0.5)
    w_hidden_b = gaussian(streams_of[16], (C, FFN), C ** -0.5, 0.5)
    w_hidden_out = gaussian(streams_of[17], (FFN, C), FFN ** -0.5, 0.25)
    w_pae = draw_w_pae(jax.random.fold_in(streams_of[20], 71), part)
    pae_bias = gaussian(streams_of[19], (BINS,), 1.0, 4.0, (), jnp.float32)
    return dict(pair_repr=pair_repr, single_repr=single_repr, residue_index=residue_index, chain_index=chain_index, complex_index=complex_index, pad_mask=pad_mask, w_query=w_query, w_key=w_key, w_value=w_value, w_gate=w_gate, w_out=w_out, w_bias=w_bias, rel_table=rel_table, w_mix_a=w_mix_a, w_mix_b=w_mix_b, w_hidden_a=w_hidden_a, w_hidden_b=w_hidden_b, w_hidden_out=w_hidden_out, w_pae=w_pae, pae_bias=pae_bias)


epsilon = 1e-05
masked_score = -1e+30

def norm_rows(values):
    center = values - lax.optimization_barrier(jnp.mean(values, axis=-1, keepdims=True))
    spread = lax.optimization_barrier(jnp.mean(center * center, axis=-1, keepdims=True))
    return center * lax.rsqrt(spread + epsilon)

def relative(res_query, chain_query, res_key, chain_key, rel_table):
    reach = (rel_table.shape[0] - 2) // 2
    offsets = jnp.clip(res_query[:, None] - res_key[None, :], -reach, reach) + reach
    bucket = jnp.where(chain_query[:, None] == chain_key[None, :], offsets, 2 * reach + 1)
    classes = jnp.arange(rel_table.shape[0], dtype=jnp.int32)
    onehot = (bucket[:, :, None] == classes[None, None, :]).astype(jnp.float32)
    return jnp.einsum('qkr,rc->qkc', onehot, rel_table.astype(jnp.float32))

def pair_tail(mixed, w_hidden_a, w_hidden_b, w_hidden_out, w_pae, pae_bias):
    width = mixed.shape[-1]
    flat = mixed.reshape(-1, width)
    normed = norm_rows(flat).astype(jnp.bfloat16)
    gate_part = jnp.dot(normed, w_hidden_a, preferred_element_type=jnp.float32)
    up_part = jnp.dot(normed, w_hidden_b, preferred_element_type=jnp.float32)
    hidden = (jax.nn.silu(gate_part) * up_part).astype(jnp.bfloat16)
    updated = flat + jnp.dot(hidden, w_hidden_out, preferred_element_type=jnp.float32)
    final = norm_rows(updated).astype(jnp.bfloat16)
    logits = jnp.dot(final, w_pae, preferred_element_type=jnp.float32) + pae_bias.astype(jnp.float32)[None, :]
    probs = jax.nn.softmax(logits, axis=-1)
    bins = w_pae.shape[1]
    centers = (jnp.arange(bins, dtype=jnp.float32) + 0.5) * (32.0 / bins)
    return lax.optimization_barrier(jnp.sum(probs * centers[None, :], axis=-1)).reshape(mixed.shape[:-1])

def reference(pair_repr, single_repr, residue_index, chain_index, complex_index, pad_mask, w_query, w_key, w_value, w_gate, w_out, w_bias, rel_table, w_mix_a, w_mix_b, w_hidden_a, w_hidden_b, w_hidden_out, w_pae, pae_bias):
    total_rows = single_repr.shape[0]
    head_count = w_bias.shape[1]
    head_size = single_repr.shape[1] // head_count
    block_rows = TOK_DEV
    normed = norm_rows(single_repr.astype(jnp.float32)).astype(jnp.bfloat16)
    queries = jnp.dot(normed, w_query, preferred_element_type=jnp.float32).astype(jnp.bfloat16)
    keys_all = jnp.dot(normed, w_key, preferred_element_type=jnp.float32).astype(jnp.bfloat16)
    values_all = jnp.dot(normed, w_value, preferred_element_type=jnp.float32).astype(jnp.bfloat16)
    gating = jax.nn.sigmoid(jnp.dot(normed, w_gate, preferred_element_type=jnp.float32))
    token_ids = jnp.arange(total_rows, dtype=jnp.int32)
    key_heads = keys_all.astype(jnp.float32).reshape(total_rows, head_count, head_size)
    value_heads = values_all.astype(jnp.float32).reshape(total_rows, head_count, head_size)

    def pair_input(offset):
        rows_pair = lax.dynamic_slice_in_dim(pair_repr, offset, block_rows, 0).astype(jnp.float32)
        res_rows = lax.dynamic_slice_in_dim(residue_index, offset, block_rows, 0)
        chain_rows = lax.dynamic_slice_in_dim(chain_index, offset, block_rows, 0)
        return rows_pair + relative(res_rows, chain_rows, residue_index, chain_index, rel_table)

    def attend(block):
        offset = (block * block_rows).astype(jnp.int32)
        pair_in = pair_input(offset)
        pair_bias = jnp.einsum('qkc,ch->hqk', norm_rows(pair_in).astype(jnp.bfloat16).astype(jnp.float32), w_bias.astype(jnp.float32)).astype(jnp.bfloat16)
        query_rows = lax.dynamic_slice_in_dim(queries, offset, block_rows, 0).astype(jnp.float32).reshape(block_rows, head_count, head_size)
        scores = jnp.einsum('qhd,khd->hqk', query_rows, key_heads) / math.sqrt(head_size) + pair_bias.astype(jnp.float32)
        row_ids = offset + jnp.arange(block_rows, dtype=jnp.int32)
        complex_rows = lax.dynamic_slice_in_dim(complex_index, offset, block_rows, 0)
        allowed = (complex_rows[:, None] == complex_index[None, :]) & ((pad_mask[None, :] == 1) | (row_ids[:, None] == token_ids[None, :]))
        scores = jnp.where(allowed[None], scores, masked_score)
        row_max = lax.optimization_barrier(jnp.max(scores, axis=-1, keepdims=True))
        expo = jnp.exp(scores - row_max)
        row_sum = lax.optimization_barrier(jnp.sum(expo, axis=-1))
        rounded = expo.astype(jnp.bfloat16).astype(jnp.float32)
        output = jnp.einsum('hqk,khd->hqd', rounded, value_heads) / row_sum[..., None]
        return output.transpose(1, 0, 2).reshape(block_rows, head_count * head_size)
    block_count = total_rows // block_rows
    attended = lax.map(attend, jnp.arange(block_count, dtype=jnp.int32)).reshape(total_rows, -1)
    refined = (single_repr.astype(jnp.float32) + jnp.dot((gating * attended).astype(jnp.bfloat16), w_out, preferred_element_type=jnp.float32)).astype(jnp.bfloat16)
    renormed = norm_rows(refined.astype(jnp.float32)).astype(jnp.bfloat16)
    factor_a = jnp.dot(renormed, w_mix_a, preferred_element_type=jnp.float32).astype(jnp.bfloat16)
    factor_b = jnp.dot(renormed, w_mix_b, preferred_element_type=jnp.float32).astype(jnp.bfloat16)

    def finish(block):
        offset = (block * block_rows).astype(jnp.int32)
        pair_in = pair_input(offset)
        rows_a = lax.dynamic_slice_in_dim(factor_a, offset, block_rows, 0).astype(jnp.float32)
        mixed = pair_in + rows_a[:, None, :] * factor_b.astype(jnp.float32)[None, :, :]
        return pair_tail(mixed, w_hidden_a, w_hidden_b, w_hidden_out, w_pae, pae_bias)
    errors = lax.map(finish, jnp.arange(block_count, dtype=jnp.int32)).reshape(total_rows, total_rows)
    return (refined, errors)
```

```python
import functools
import math

import jax
import jax.numpy as jnp
from jax import lax
from jax.experimental import pallas as pl
from jax.experimental.pallas import tpu as pltpu
from jax.sharding import PartitionSpec as P

epsilon = 1e-05
masked_score = -1e30
chain_step = 65536.0
f32 = jnp.float32
bf16 = jnp.bfloat16


def norm_rows(values):
    center = values - jnp.mean(values, axis=-1, keepdims=True)
    spread = jnp.mean(center * center, axis=-1, keepdims=True)
    return center * lax.rsqrt(spread + epsilon)


def mm(a, b):
    return jnp.dot(a, b, preferred_element_type=f32)


def mm_nt(a, b):
    return lax.dot_general(a, b, (((1,), (1,)), ((), ())), preferred_element_type=f32)


def column(row):
    m = row.shape[1]
    pick = lax.broadcasted_iota(jnp.int32, (m, m), 0) == lax.broadcasted_iota(jnp.int32, (m, m), 1)
    return jnp.sum(jnp.where(pick, row, 0.0), axis=1, keepdims=True)


def bucket_onehot(diff, classes):
    reach = (classes - 2) // 2
    same = jnp.abs(diff) < 0.5 * chain_step
    bucket = jnp.where(same, jnp.clip(diff, -reach, reach) + reach, 2.0 * reach + 1.0)
    lanes = lax.broadcasted_iota(jnp.int32, bucket.shape, bucket.ndim - 1).astype(f32)
    return jnp.where(bucket == lanes, 1.0, 0.0).astype(bf16)


def kernel(
    n,
    heads,
    pair_h, single_h, res_h, chain_h, complex_h, pad_h,
    wq_h, wk_h, wv_h, wg_h, wo_h, wb_h, rel_h, wma_h, wmb_h, wha_h, whb_h, who_h, wp_h, pb_h,
    refined_ref, errors_ref,
    pair_v, single_v, res_v, chain_v, complex_v, pad_v,
    wq_v, wk_v, wv_v, wg_v, wo_v, wb_v, rel_v, wma_v, wmb_v, wha_v, whb_v, who_v, wp_v, pb_v,
    code_v, ccol_v, bias_s, bias_r, single_r, pair_r, b_s, b_r, a_v, pin_v, score_v,
    local_sem, own_sem, send_sem, recv_sem,
):
    me = lax.axis_index("rows")
    count, rows, width = pair_h.shape
    classes = rel_h.shape[0]
    inner = single_h.shape[1]
    head_size = inner // heads
    first = pl.multiple_of(me * rows, rows)

    hbm = (pair_h, single_h, res_h, chain_h, complex_h, pad_h, wq_h, wk_h, wv_h, wg_h, wo_h,
           wb_h, rel_h, wma_h, wmb_h, wha_h, whb_h, who_h, wp_h, pb_h)
    vmem = (pair_v, single_v, res_v, chain_v, complex_v, pad_v, wq_v, wk_v, wv_v, wg_v, wo_v,
            wb_v, rel_v, wma_v, wmb_v, wha_v, whb_v, who_v, wp_v, pb_v)
    (PAIR, SINGLE, RES, CHAIN, COMPLEX, PAD, WQ, WK, WV, WG, WO, WB, REL, WMA, WMB, WHA, WHB,
     WHO, WP, PB) = range(len(hbm))
    loads = [pltpu.make_async_copy(h, v, local_sem.at[i]) for i, (h, v) in enumerate(zip(hbm, vmem))]

    barrier = pltpu.get_barrier_semaphore()

    def greet(s, _):
        pl.semaphore_signal(
            barrier, inc=1, device_id={"rows": lax.rem(me + s, n)},
            device_id_type=pl.DeviceIdType.MESH,
        )
        return 0

    lax.fori_loop(1, n, greet, 0)
    for i in (RES, CHAIN, REL, WB, PAIR, SINGLE, COMPLEX, PAD, WQ, WG, WK, WV, WO, WMB, WMA,
              WHA, WHB, WHO, WP, PB):
        loads[i].start()

    for i in (RES, CHAIN, COMPLEX):
        loads[i].wait()
    step = min(count, 128)
    for k in range(0, count, step):
        code = chain_v[:, k:k + step].astype(f32) * chain_step + res_v[:, k:k + step].astype(f32)
        code_v[k:k + step, :] = jnp.broadcast_to(column(code), (step, 128))
        ccol_v[k:k + step, :] = jnp.broadcast_to(
            column(complex_v[:, k:k + step].astype(f32)), (step, 128))

    for i in (REL, WB, PAIR):
        loads[i].wait()
    rel = rel_v[...]
    spots = rows * heads
    tile_h = jnp.where(
        lax.broadcasted_iota(jnp.int32, (heads, spots), 1) % heads
        == lax.broadcasted_iota(jnp.int32, (heads, spots), 0), 1.0, 0.0).astype(bf16)
    w_tiled = lax.dot_general(
        wb_v[...], tile_h, (((0,), (0,)), ((), ())), preferred_element_type=f32).astype(bf16)
    code_keys = code_v[pl.ds(first, rows), :classes]

    def bias_block(j, _):
        at = pl.multiple_of(j * step, step)
        code_i = code_v[pl.ds(at, step), :classes]
        diff = code_i[:, None, :] - code_keys[None, :, :]
        hot = bucket_onehot(diff.reshape(step * rows, classes), classes)
        cells = mm(hot, rel) + pair_v[pl.ds(at, step)].astype(f32).reshape(step * rows, width)
        out = mm(norm_rows(cells).astype(bf16), w_tiled)
        out = out.reshape(step // rows, rows, rows, spots)
        lane_q = lax.broadcasted_iota(jnp.int32, (1, 1, spots), 2) // heads
        total = jnp.where(lane_q == 0, out[:, 0], 0.0)
        for q in range(1, rows):
            total = jnp.where(lane_q == q, out[:, q], total)
        bias_s[pl.ds(pl.multiple_of(j * (step // rows), step // rows), step // rows)] = total.astype(bf16)
        return 0

    lax.fori_loop(0, count // step, bias_block, 0, unroll=count == step)
    loads[SINGLE].wait()

    pl.semaphore_wait(barrier, n - 1)

    def remote(src, dst, i, peer):
        return pltpu.make_async_remote_copy(
            src_ref=src, dst_ref=dst, send_sem=send_sem.at[i], recv_sem=recv_sem.at[i],
            device_id={"rows": peer}, device_id_type=pl.DeviceIdType.MESH)

    def send_single(s, _):
        peer = lax.rem(me + s, n)
        remote(single_v, single_r.at[me], 0, peer).start()
        return 0

    def send_bias(s, _):
        peer = lax.rem(me + s, n)
        remote(bias_s.at[peer], bias_r.at[me], 1, peer).start()
        return 0

    def send_pair(s, _):
        peer = lax.rem(me + s, n)
        remote(pair_v.at[pl.ds(peer * rows, rows)], pair_r.at[:, me], 2, peer).start()
        return 0

    lax.fori_loop(1, n, send_single, 0)
    lax.fori_loop(1, n, send_bias, 0)
    lax.fori_loop(1, n, send_pair, 0)
    own = (
        pltpu.make_async_copy(single_v, single_r.at[me], own_sem.at[0]),
        pltpu.make_async_copy(bias_s.at[me], bias_r.at[me], own_sem.at[1]),
        pltpu.make_async_copy(pair_v.at[pl.ds(first, rows)], pair_r.at[:, me], own_sem.at[2]),
    )
    for copy in own:
        copy.start()

    mine = single_v[...].astype(f32)
    normed = norm_rows(mine).astype(bf16)
    loads[WQ].wait()
    queries = mm(normed, wq_v[...]).astype(bf16).astype(f32)
    loads[WG].wait()
    gating = jax.nn.sigmoid(mm(normed, wg_v[...]))
    head_of = lax.broadcasted_iota(jnp.int32, (heads, inner), 1) // head_size
    own_head = head_of == lax.broadcasted_iota(jnp.int32, (heads, inner), 0)
    q_wide = jnp.concatenate(
        [jnp.where(own_head, queries[q:q + 1, :], 0.0) for q in range(rows)], axis=0).astype(bf16)

    def rel_block(q, _):
        diff = code_v[pl.ds(first + q, 1), :classes] - code_v[:, :classes]
        pin_v[q] = mm(bucket_onehot(diff, classes), rel)
        return 0

    lax.fori_loop(0, rows, rel_block, 0, unroll=count == step)

    loads[WK].wait()
    loads[WV].wait()
    own[0].wait()
    landed = single_r.at[pl.ds(0, n - 1)]
    pltpu.make_async_copy(landed, landed, recv_sem.at[0]).wait()
    every = norm_rows(single_r[...].astype(f32).reshape(count, inner)).astype(bf16)
    keys = mm(every, wk_v[...]).astype(bf16)
    values = mm(every, wv_v[...]).astype(bf16)
    scores = mm_nt(q_wide, keys) / math.sqrt(head_size)
    loads[PAD].wait()
    key_ids = lax.broadcasted_iota(jnp.int32, (1, count), 1)
    complex_row = complex_v[...].astype(f32)
    real = pad_v[...] == 1
    own[1].wait()
    landed = bias_r.at[pl.ds(0, n - 1)]
    pltpu.make_async_copy(landed, landed, recv_sem.at[1]).wait()
    eye = jnp.where(
        lax.broadcasted_iota(jnp.int32, (spots, spots), 0)
        == lax.broadcasted_iota(jnp.int32, (spots, spots), 1), 1.0, 0.0).astype(bf16)
    arrived = bias_r[...].astype(f32).reshape(count, spots).astype(bf16)
    scores = scores + mm_nt(eye, arrived)
    for q in range(rows):
        allowed = (ccol_v[pl.ds(first + q, 1), 0:1] == complex_row) & (real | (key_ids == first + q))
        part = scores[q * heads:(q + 1) * heads, :]
        score_v[q * heads:(q + 1) * heads, :] = jnp.where(allowed, part, masked_score)
    scores = score_v[...]
    expo = jnp.exp(scores - jnp.max(scores, axis=-1, keepdims=True))
    total = jnp.sum(expo, axis=-1, keepdims=True)
    mixed_heads = mm(expo.astype(bf16), values) / total
    attended = jnp.concatenate(
        [jnp.sum(jnp.where(own_head, mixed_heads[q * heads:(q + 1) * heads, :], 0.0),
                 axis=0, keepdims=True) for q in range(rows)], axis=0)
    loads[WO].wait()
    refined = (mine + mm((gating * attended).astype(bf16), wo_v[...])).astype(bf16)
    renormed = norm_rows(refined.astype(f32)).astype(bf16)
    loads[WMB].wait()
    b_s[...] = mm(renormed, wmb_v[...]).astype(bf16)
    b_r[me] = b_s[...]
    loads[WMA].wait()
    a_v[...] = mm(renormed, wma_v[...]).astype(bf16).astype(f32)

    def send_b(s, _):
        remote(b_s, b_r.at[me], 3, lax.rem(me + s, n)).start()
        return 0

    lax.fori_loop(1, n, send_b, 0)
    refined_ref[...] = refined

    own[2].wait()
    landed = pair_r.at[:, pl.ds(0, n - 1)]
    pltpu.make_async_copy(landed, landed, recv_sem.at[2]).wait()

    def add_block(q, _):
        pin_v[q] = pin_v[q] + pair_r[q].astype(f32).reshape(count, width)
        return 0

    lax.fori_loop(0, rows, add_block, 0, unroll=count == step)
    for i in (WHA, WHB, WHO, WP, PB):
        loads[i].wait()
    bins = wp_v.shape[0]
    bias_col = column(pb_v[...])
    centers = (lax.broadcasted_iota(jnp.int32, (bins, 1), 0).astype(f32) + 0.5) * (32.0 / bins)
    landed = b_r.at[pl.ds(0, n - 1)]
    pltpu.make_async_copy(landed, landed, recv_sem.at[3]).wait()

    def tail(c, _):
        at = pl.multiple_of(c * step, step)
        tile = pl.multiple_of(c * (step // rows), step // rows)
        factor_b = b_r[pl.ds(tile, step // rows)].astype(f32).reshape(step, width)
        found = []
        for q in range(rows):
            flat = pin_v[q, pl.ds(at, step), :] + a_v[q:q + 1, :] * factor_b
            x = norm_rows(flat).astype(bf16)
            gate = mm(x, wha_v[...])
            up = mm(x, whb_v[...])
            half = 0.5 * gate
            hidden = ((half + half * jnp.tanh(half)) * up).astype(bf16)
            updated = flat + mm(hidden, who_v[...])
            final = norm_rows(updated).astype(bf16)
            logits = mm_nt(wp_v[...], final) + bias_col
            expo = jnp.exp(logits - jnp.max(logits, axis=0, keepdims=True))
            found.append(jnp.sum(expo * centers, axis=0, keepdims=True)
                         / jnp.sum(expo, axis=0, keepdims=True))
        errors_ref[:, pl.ds(at, step)] = jnp.concatenate(found, axis=0)
        return 0

    lax.fori_loop(0, count // step, tail, 0, unroll=count == step)

    for i, buf in enumerate((single_r, bias_r, None, b_r)):
        sent = pair_r.at[:, pl.ds(0, n - 1)] if buf is None else buf.at[pl.ds(0, n - 1)]
        pltpu.make_async_copy(sent, sent, send_sem.at[i]).wait()


def on_device(n, pair_repr, single_repr, residue_index, chain_index, complex_index, pad_mask,
              w_query, w_key, w_value, w_gate, w_out, w_bias, rel_table, w_mix_a, w_mix_b,
              w_hidden_a, w_hidden_b, w_hidden_out, w_pae, pae_bias):
    count, rows, width = pair_repr.shape
    inner = single_repr.shape[1]
    heads = w_bias.shape[1]
    args = (pair_repr, single_repr, residue_index[None], chain_index[None], complex_index[None],
            pad_mask[None], w_query, w_key, w_value, w_gate, w_out, w_bias.T, rel_table,
            w_mix_a, w_mix_b, w_hidden_a, w_hidden_b, w_hidden_out, w_pae.T, pae_bias[None])
    spots = rows * heads
    scratch = [pltpu.VMEM(a.shape, a.dtype) for a in args] + [
        pltpu.VMEM((count, 128), f32),
        pltpu.VMEM((count, 128), f32),
        pltpu.VMEM((n, rows, spots), bf16),
        pltpu.VMEM((n, rows, spots), bf16),
        pltpu.VMEM((n, rows, inner), bf16),
        pltpu.VMEM((rows, n, rows, width), bf16),
        pltpu.VMEM((rows, width), bf16),
        pltpu.VMEM((n, rows, width), bf16),
        pltpu.VMEM((rows, width), f32),
        pltpu.VMEM((rows, count, width), f32),
        pltpu.VMEM((spots, count), f32),
        pltpu.SemaphoreType.DMA((len(args),)),
        pltpu.SemaphoreType.DMA((3,)),
        pltpu.SemaphoreType.DMA((4,)),
        pltpu.SemaphoreType.DMA((4,)),
    ]
    return pl.pallas_call(
        functools.partial(kernel, n, heads),
        out_shape=(
            jax.ShapeDtypeStruct((rows, inner), bf16),
            jax.ShapeDtypeStruct((rows, count), f32),
        ),
        in_specs=[pl.BlockSpec(memory_space=pltpu.HBM)] * len(args),
        out_specs=[pl.BlockSpec(memory_space=pltpu.VMEM)] * 2,
        scratch_shapes=scratch,
        compiler_params=pltpu.CompilerParams(
            collective_id=0, has_side_effects=True, vmem_limit_bytes=60 * 1024 * 1024),
        name="confidence",
    )(*args)


def solution(mesh):
    placed = (
        P("groups", "rows", None),
        P(("groups", "rows"), None),
        P("groups"),
        P("groups"),
        P("groups"),
        P("groups"),
    ) + (P(),) * 14
    return jax.shard_map(
        functools.partial(on_device, mesh.shape["rows"]),
        mesh=mesh,
        in_specs=placed,
        out_specs=(P(("groups", "rows"), None), P(("groups", "rows"), None)),
        check_vma=False,
    )
```
